32 devices in a mesh: lat: 8 (over z, core), rad: 4 (over y, x).
Axes of the slice: x: 2, y: 2, z: 4, core: 2. Of those that a mesh axis runs over, the one named last changes fastest.
Arguments:
- residual: float32 [3, 32, 64, 256], P(None, 'rad', 'lat'), may hold values from -30 to 30
- prev_basis: float32 [4, 3, 32, 64, 256], P(None, None, 'rad', 'lat'), may hold values from -30 to 30
- layer_ids: int32 [16, 32, 128], P('rad', 'lat'), may hold values from 0 to 7
- viscosity: float32 [8], replicated, may hold values from 0.1 to 1
- shifts: float32 [4], replicated, may hold values from 0.3 to 2
Outputs:
- new_basis: float32 [4, 3, 32, 64, 256], P(None, None, 'rad', 'lat')
- gram_matrix: float32 [9, 9], replicated
The draws below stay inside these ranges and needn't reach their ends.
All inputs are finite; a program needn't handle non-finite values.
Results may differ from the reference program's by a relative error of at most 0.00019.
Values sent between devices are 32-bit elements; how exact they have to be, the bound alone decides.
A program may use at most 128 MiB of HBM per device.

```python
import math
import jax
import jax.numpy as jnp
from jax import lax

COMP = 3
S = 4
PREV = 4
LAYERS = 8
ER = 4
EY = 128
BASIS = 9
NRE = 16
NXE = 32
NRN = 32
NXN = 64
NYN = 256
N_RAD = 4


def ramp_field(key, leading):
    full_shape = (leading, COMP, NRN, NXN, NYN)
    radial = (jnp.arange(NRN, dtype=jnp.float32) / NRN)[:, None, None]
    lateral = (jnp.arange(NXN, dtype=jnp.float32) / NXN)[None, :, None]
    across = (jnp.arange(NYN, dtype=jnp.float32) / NYN)[None, None, :]
    smooth = jnp.sin(6.0 * radial + 4.0 * lateral + 3.0 * across + 0.5)
    coef_key = jax.random.fold_in(key, 7)
    coefs = jax.random.truncated_normal(coef_key, -2.0, 2.0, (leading, COMP, 1, 1, 1), jnp.float32)
    noise_vals = jax.random.truncated_normal(key, -4.0, 4.0, full_shape, jnp.float32)
    amplitude = 3.0 ** (radial + lateral - 1.0)
    return (amplitude * (noise_vals + coefs * smooth)).astype(jnp.float32)


def draw_residual(key, part):
    return ramp_field(jax.random.fold_in(key, 11), 1)[0]


def draw_prev_basis(key, part):
    return ramp_field(jax.random.fold_in(key, 23), PREV)


def touch_ends(values, stream_key, low, largest):
    spot = [jax.random.randint(jax.random.fold_in(stream_key, axis), (), 0, length) for axis, length in enumerate(values.shape)]
    widest = values.shape.index(max(values.shape))
    beside = spot[:widest] + [(spot[widest] + 1) % values.shape[widest]] + spot[widest + 1:]
    return values.at[tuple(spot)].set(low).at[tuple(beside)].set(largest)


def setup_inputs(seed: int = 0) -> dict:
    splits = jax.random.split(jax.random.key(seed), 6)
    residual = draw_residual(jax.random.fold_in(splits[5], 71), 0)
    prev_basis = draw_prev_basis(jax.random.fold_in(splits[5], 71), 0)
    layer_ids = touch_ends(jax.random.randint(splits[2], (NRE, NXE, EY), 0, LAYERS), jax.random.fold_in(splits[2], 1), 0, LAYERS - 1).astype(jnp.int32)
    viscosity = jnp.clip(jnp.exp(jax.random.uniform(splits[3], (LAYERS,), jnp.float32, math.log(0.1), math.log(1.0))), 0.1, 1.0)
    shifts = jnp.clip(jax.random.uniform(splits[4], (S,), jnp.float32, 0.3, 2.0), 0.3, 2.0)
    return {"residual": residual, "prev_basis": prev_basis, "layer_ids": layer_ids, "viscosity": viscosity, "shifts": shifts}


stiff_line = ((7.0 / 3, -8.0 / 3, 1.0 / 3), (-8.0 / 3, 16.0 / 3, -8.0 / 3), (1.0 / 3, -8.0 / 3, 7.0 / 3))
mass_line = ((4.0 / 30, 2.0 / 30, -1.0 / 30), (2.0 / 30, 16.0 / 30, 2.0 / 30), (-1.0 / 30, 2.0 / 30, 4.0 / 30))


def contract(line_table, element_vals, axis_pos):
    pieces = [lax.index_in_dim(element_vals, j, axis_pos, keepdims=False) for j in range(3)]
    row_terms = [line_table[i][0] * pieces[0] + line_table[i][1] * pieces[1] + line_table[i][2] * pieces[2] for i in range(3)]
    return jnp.stack(row_terms, axis_pos)


def split_local(field_in, axis_pos):
    el_count = field_in.shape[axis_pos] // 2 - 1
    return jnp.stack([lax.slice_in_dim(field_in, k, k + 2 * el_count - 1, 2, axis_pos) for k in range(3)], 0)


def join_local(element_vals, axis_pos):
    lower_side = element_vals[0]
    middle = element_vals[1]
    upper_side = element_vals[2]
    el_count = lower_side.shape[axis_pos]
    even_nodes = lax.slice_in_dim(lower_side, 1, el_count, 1, axis_pos) + lax.slice_in_dim(upper_side, 0, el_count - 1, 1, axis_pos)
    odd_nodes = lax.slice_in_dim(middle, 1, el_count, 1, axis_pos)
    alternated = jnp.stack([even_nodes, odd_nodes], axis_pos + 1)
    new_shape = list(even_nodes.shape)
    new_shape[axis_pos] = 2 * (el_count - 1)
    return alternated.reshape(new_shape)


def stiffness(field_in, viscous):
    padded = jnp.pad(field_in, ((0, 0), (0, 0), (0, 0), (2, 2)))
    element_vals = split_local(padded, 1)
    element_vals = split_local(element_vals, 3)
    element_vals = split_local(element_vals, 5)
    along_y = contract(mass_line, element_vals, 0)
    mass_rx = contract(mass_line, along_y, 1)
    term_r = contract(stiff_line, mass_rx, 2)
    term_x = contract(mass_line, contract(stiff_line, along_y, 1), 2)
    term_y = contract(stiff_line, contract(mass_line, contract(mass_line, element_vals, 2), 1), 0)
    viscous_wide = jnp.pad(viscous, ((0, 0), (0, 0), (1, 0)))
    weighted = (term_r + term_x + term_y) * viscous_wide
    assembled = join_local(weighted, 5)
    assembled = join_local(assembled, 3)
    return join_local(assembled, 1)


def reference(residual, prev_basis, layer_ids, viscosity, shifts):
    viscous = jnp.take(viscosity, layer_ids)
    eta_pad = jnp.pad(viscous, ((1, 1), (1, 1), (0, 0)))

    def apply_op(field_in):
        padded = jnp.pad(field_in, ((0, 0), (2, 2), (2, 2), (0, 0)))

        def slab_apply(j):
            slab_nodes = lax.dynamic_slice_in_dim(padded, j * (2 * ER), 2 * ER + 4, 1)
            slab_visc = lax.dynamic_slice_in_dim(eta_pad, j * ER, ER + 1, 0)
            return stiffness(slab_nodes, slab_visc[:, :NXE + 1])

        pieces = lax.map(slab_apply, jnp.arange(N_RAD, dtype=jnp.int32))
        return jnp.transpose(pieces, (1, 0, 2, 3, 4)).reshape(field_in.shape)

    vectors = [residual]
    for k in range(S):
        vectors.append(apply_op(vectors[-1]) - shifts[k] * vectors[-1])
    new_basis = jnp.stack(vectors[1:], 0)
    stacked = jnp.concatenate([prev_basis, jnp.stack(vectors, 0)], 0).reshape(BASIS, -1)
    gram_matrix = jnp.dot(stacked, stacked.T, precision=lax.Precision.HIGHEST, preferred_element_type=jnp.float32)
    gram_matrix = gram_matrix / (COMP * NRN * NXN * NYN)
    return new_basis, gram_matrix
```

```python
import functools

import jax
import jax.numpy as jnp
from jax import lax
from jax.experimental import pallas as pl
from jax.experimental.pallas import tpu as pltpu
from jax.sharding import PartitionSpec as P

MESH = pl.DeviceIdType.MESH
F32 = jnp.float32

mass = (1.0 / 36, 1.0 / 12, 1.0 / 45)
stiff = (0.0, 1.0, 4.0 / 3)

DIRS = ((-1, -1), (-1, 0), (-1, 1), (0, -1), (0, 1), (1, -1), (1, 0), (1, 1))
SLOT = {d: i for i, d in enumerate(DIRS)}
R_DIRS = {(-1, 0): 0, (1, 0): 1}
X_DIRS = {(0, -1): 0, (0, 1): 1}
C_DIRS = {(-1, -1): 0, (-1, 1): 1, (1, -1): 2, (1, 1): 3}
FIRST = ((-1, 0), (0, -1), (-1, -1))
LAST = ((1, 0), (0, 1), (1, 1))


def weight(a, b, c):
    return (
        stiff[a] * mass[b] * mass[c] + mass[a] * stiff[b] * mass[c] + mass[a] * mass[b] * stiff[c]
    )


def forward(u0, u1, u2):
    total = u0 + u2
    twice = u1 + u1
    return total + (twice + twice), u0 - u2, total - twice


def backward(m0, m1, m2):
    both = m0 + m2
    half = m0 + m0 - m2
    return both + m1, half + half, both - m1


def kernel(
    n_lat,
    n_rad,
    n_steps,
    n_prev,
    comps,
    res_ref,
    prev_ref,
    ids_ref,
    visc_ref,
    shift_ref,
    out_ref,
    gram_ref,
    stage,
    back,
    work,
    vec,
    ghost_r,
    ghost_x,
    ghost_c,
    scaled,
    send_r,
    send_x,
    send_c,
    recv_r,
    recv_x,
    recv_c,
    gram_send,
    gram_recv,
    in_sem,
    out_sem,
    send_sem,
    recv_sem,
    gram_sems,
):
    n_dev = n_lat * n_rad
    lat = lax.axis_index("lat")
    rad = lax.axis_index("rad")
    me = lat * n_rad + rad
    rows = res_ref.shape[0]
    half_y = res_ref.shape[1] // 2
    n_vec = n_prev + n_steps + 1

    res_copy = pltpu.make_async_copy(res_ref, stage.at[n_prev], in_sem.at[0])
    res_copy.start()
    prev_copy = pltpu.make_async_copy(prev_ref, stage.at[pl.ds(0, n_prev)], in_sem.at[1])
    prev_copy.start()

    recv_r[...] = jnp.zeros_like(recv_r)
    recv_x[...] = jnp.zeros_like(recv_x)
    recv_c[...] = jnp.zeros_like(recv_c)

    barrier = pltpu.get_barrier_semaphore()

    def other(d):
        t = lax.rem(me + d, n_dev)
        return {"lat": t // n_rad, "rad": lax.rem(t, n_rad)}

    def greet(d, carry):
        pl.semaphore_signal(barrier, inc=1, device_id=other(d), device_id_type=MESH)
        return carry

    lax.fori_loop(1, n_dev, greet, 0)

    sub = lax.broadcasted_iota(jnp.int32, (8, half_y), 0)
    lane = lax.broadcasted_iota(jnp.int32, (8, half_y), 1)
    upper = sub >= 4
    ex = lax.rem(sub, 4)
    first_x = ex == 0
    last_x = ex == 3
    corner0 = sub == 0
    corner3 = sub == 3
    corner4 = sub == 4
    corner7 = sub == 7
    has_up = rad < n_rad - 1
    has_right = lat < n_lat - 1
    up_f = jnp.where(has_up, 1.0, 0.0).astype(F32)
    right_f = jnp.where(has_right, 1.0, 0.0).astype(F32)
    both_f = up_f * right_f

    def roll_s(v, k):
        return pltpu.roll(v, k % 8, 0)

    def keep(mask, v):
        return jnp.where(mask, v, 0.0)

    src = lax.broadcasted_iota(jnp.int32, (2 * half_y, 2 * half_y), 0)
    dst = lax.broadcasted_iota(jnp.int32, (2 * half_y, 2 * half_y), 1)
    split_perm = jnp.where(
        src == jnp.where(dst < half_y, 2 * dst, 2 * (dst - half_y) + 1), 1.0, 0.0
    ).astype(F32)
    join_perm = jnp.where(
        dst == jnp.where(src < half_y, 2 * src, 2 * (src - half_y) + 1), 1.0, 0.0
    ).astype(F32)

    def exact_dot(a, b):
        return jnp.dot(a, b, precision=lax.Precision.HIGHEST, preferred_element_type=F32)

    def split_columns(i):
        z = exact_dot(stage[i], split_perm)
        work[i, 0] = z[:, :half_y]
        work[i, 1] = z[:, half_y:]

    def native(c, ro, p, h):
        return pl.ds(c * 64 + (4 * h + ro) * 8 + p, 4, stride=2)

    kinds = {}
    for a in range(3):
        for b in range(3):
            for c in range(3):
                key = tuple(sorted((a, b, c)))
                if key != (0, 0, 0) and key not in kinds:
                    kinds[key] = len(kinds)
    for e in range(2):
        ids = jnp.concatenate([ids_ref[e], ids_ref[2 + e]], 0)
        eta = jnp.zeros((8, half_y), F32)
        for layer in range(visc_ref.shape[0]):
            eta = eta + jnp.where(ids == layer, visc_ref[layer], 0.0)
        for key, i in kinds.items():
            scaled[e, i] = eta * weight(*key)

    def copy_of(step, d):
        if d in R_DIRS:
            a, b = send_r.at[step, R_DIRS[d]], recv_r.at[step, R_DIRS[d]]
        elif d in X_DIRS:
            a, b = send_x.at[step, X_DIRS[d]], recv_x.at[step, X_DIRS[d]]
        else:
            a, b = send_c.at[step, C_DIRS[d]], recv_c.at[step, C_DIRS[d]]
        return pltpu.make_async_remote_copy(
            src_ref=a,
            dst_ref=b,
            send_sem=send_sem.at[step, SLOT[d]],
            recv_sem=recv_sem.at[step, SLOT[d]],
            device_id={"lat": lat + d[1], "rad": rad + d[0]},
            device_id_type=MESH,
        )

    def inside(dr, dx):
        ok = None
        for pos, step, count in ((rad, dr, n_rad), (lat, dx, n_lat)):
            if step:
                one = (pos > 0) if step < 0 else (pos < count - 1)
                ok = one if ok is None else jnp.logical_and(ok, one)
        return ok

    order = ((-1, -1), (1, 1), (-1, 1), (1, -1), (1, 0), (-1, 0), (0, 1), (0, -1))

    def dirs_of(step):
        wanted = FIRST if step == 0 else (LAST if step == n_steps else DIRS)
        return [d for d in order if d in wanted]

    def start_round(step):
        for d in dirs_of(step):

            @pl.when(inside(*d))
            def _(d=d):
                copy_of(step, d).start()

    def finish_round(step):
        for d in dirs_of(step):

            @pl.when(inside(-d[0], -d[1]))
            def _(d=d):
                copy_of(step, d).wait_recv()

    def pack_x(vals, at):
        out = None
        for ro in range(4):
            moved = roll_s(vals[ro], ro - at)
            out = moved if out is None else jnp.where(ex == ro, moved, out)
        return out

    def apply(k, c):
        s = shift_ref[k]
        cur = k % 2
        new = 1 - cur
        u = {}
        gx = {}
        for q in range(2):
            for ro in range(4):
                gx[ro, q] = ghost_x[cur, c, ro, q]
                for p in range(2):
                    u[ro, p, q] = vec[cur, c, ro, p, q]
            gx[4, q] = jnp.where(upper, ghost_c[cur, c, q], roll_s(gx[0, q], 4))
            for p in range(2):
                u[4, p, q] = jnp.where(upper, ghost_r[cur, c, p, q], roll_s(u[0, p, q], 4))
            for ro in range(5):
                u[ro, 2, q] = jnp.where(last_x, gx[ro, q], roll_s(u[ro, 0, q], -1))
        res = {}
        for e in range(2):
            t = {}
            for p in range(3):
                for q in range(2):
                    t[0, p, q], t[1, p, q], t[2, p, q] = forward(
                        u[2 * e, p, q], u[2 * e + 1, p, q], u[2 * e + 2, p, q]
                    )
            w = {}
            for a in range(3):
                x = {}
                for q in range(2):
                    x[0, q], x[1, q], x[2, q] = forward(t[a, 0, q], t[a, 1, q], t[a, 2, q])
                for b in range(3):
                    nxt = keep(lane != half_y - 1, pltpu.roll(x[b, 0], half_y - 1, 1))
                    m = list(forward(x[b, 0], x[b, 1], nxt))
                    for j in range(3):
                        key = tuple(sorted((a, b, j)))
                        if key in kinds:
                            m[j] = m[j] * scaled[e, kinds[key]]
                        else:
                            m[j] = None
                    if m[0] is None:
                        r0 = m[1] + m[2]
                        r1 = -(m[2] + m[2])
                        r2 = m[2] - m[1]
                    else:
                        r0, r1, r2 = backward(*m)
                    x[b, 0] = r0 + keep(lane != 0, pltpu.roll(r2, 1, 1))
                    x[b, 1] = r1
                for q in range(2):
                    w[a, 0, q], w[a, 1, q], w[a, 2, q] = backward(x[0, q], x[1, q], x[2, q])
            for p in range(3):
                for q in range(2):
                    r = backward(w[0, p, q], w[1, p, q], w[2, p, q])
                    for i in range(3):
                        key = (2 * e + i, p, q)
                        res[key] = res[key] + r[i] if key in res else r[i]
        px = {}
        for q in range(2):
            for ro in range(5):
                edge = res[ro, 2, q]
                px[ro, q] = edge
                res[ro, 0, q] = res[ro, 0, q] + keep(ex != 0, roll_s(edge, 1))
            for p in range(2):
                res[0, p, q] = res[0, p, q] + keep(upper, roll_s(res[4, p, q], 4))
            px[0, q] = px[0, q] + keep(upper, roll_s(px[4, q], 4))
        step = k + 1
        last = step == n_steps
        for q in range(2):
            i = 2 * c + q
            row = slice(i, i + 1)
            send_r[step, 1, i] = jnp.where(upper, res[4, 1, q], roll_s(res[4, 0, q], 4))
            send_r[step, 1, 2 * comps, row] = px[4, q][7:8]
            send_x[step, 1, i] = pack_x([px[ro, q] for ro in range(4)], 3)
            send_x[step, 1, 2 * comps, row] = px[4, q][7:8]
            send_c[step, 3, row] = px[4, q][7:8]
            if not last:
                send_r[step, 0, i] = jnp.where(upper, roll_s(res[0, 1, q], 4), res[0, 0, q])
                send_r[step, 0, 2 * comps, row] = px[0, q][3:4]
                send_x[step, 0, i] = pack_x([res[ro, 0, q] for ro in range(4)], 0)
                send_x[step, 0, 2 * comps, row] = res[4, 0, q][4:5]
                send_c[step, 0, row] = res[0, 0, q][0:1]
                send_c[step, 1, row] = px[0, q][3:4]
                send_c[step, 2, row] = res[4, 0, q][4:5]
            for ro in range(4):
                for p in range(2):
                    vec[new, c, ro, p, q] = res[ro, p, q] - s * u[ro, p, q]
                if not last:
                    ghost_x[new, c, ro, q] = px[ro, q] - s * gx[ro, q]
            if not last:
                for p in range(2):
                    ghost_r[new, c, p, q] = res[4, p, q] - s * u[4, p, q]
                ghost_c[new, c, q] = px[4, q] - s * gx[4, q]

    def absorb(step, c):
        new = step % 2
        first, last = step == 0, step == n_steps
        for q in range(2):
            i = 2 * c + q
            row = slice(i, i + 1)

            def spot(ref_row, mask):
                return keep(mask, jnp.broadcast_to(ref_row, (8, half_y)))

            if not first:
                from_low = recv_r[step, 1, i]
                from_left = recv_x[step, 1, i]
                corner = spot(recv_c[step, 3, row], corner0)
                vec[new, c, 0, 0, q] += (
                    keep(~upper, from_low) + keep(first_x, from_left) + corner
                )
                vec[new, c, 0, 1, q] += keep(~upper, roll_s(from_low, 4))
                for ro in range(1, 4):
                    vec[new, c, ro, 0, q] += keep(first_x, roll_s(from_left, -ro))
            if not last:
                from_up = recv_r[step, 0, i]
                from_right = recv_x[step, 0, i]
                add0 = keep(upper, roll_s(from_up, 4))
                add1 = keep(upper, from_up)
                edge = keep(last_x, roll_s(from_right, 3))
                far = (
                    spot(recv_r[step, 0, 2 * comps, row], corner7)
                    + spot(recv_x[step, 0, 2 * comps, row], corner7)
                    + spot(recv_c[step, 0, row], corner7)
                )
                if not first:
                    add0 = (
                        add0
                        + spot(recv_x[step, 1, 2 * comps, row], corner4)
                        + spot(recv_c[step, 1, row], corner4)
                    )
                    edge = (
                        edge
                        + spot(recv_r[step, 1, 2 * comps, row], corner3)
                        + spot(recv_c[step, 2, row], corner3)
                    )
                    add0 = add0 + ghost_r[new, c, 0, q]
                    add1 = add1 + ghost_r[new, c, 1, q]
                    edge = edge + ghost_x[new, c, 0, q]
                    far = far + ghost_c[new, c, q]
                ghost_r[new, c, 0, q] = add0 * up_f
                ghost_r[new, c, 1, q] = add1 * up_f
                ghost_x[new, c, 0, q] = edge * right_f
                ghost_c[new, c, q] = far * both_f
                for ro in range(1, 4):
                    edge = keep(last_x, roll_s(from_right, 3 - ro))
                    if not first:
                        edge = edge + ghost_x[new, c, ro, q]
                    ghost_x[new, c, ro, q] = edge * right_f

    def to_native(k):
        cur = k % 2
        for c in range(comps):
            for ro in range(4):
                for p in range(2):
                    for q in range(2):
                        v = vec[cur, c, ro, p, q]
                        for h in range(2):
                            work[n_prev + k, q, native(c, ro, p, h), :] = v[4 * h : 4 * h + 4]

    def out_copy(k):
        return pltpu.make_async_copy(back.at[k - 1], out_ref.at[k - 1], out_sem.at[k - 1])

    def write_out(k):
        z = jnp.concatenate([work[n_prev + k, 0], work[n_prev + k, 1]], 1)
        back[k - 1] = exact_dot(z, join_perm)
        out_copy(k).start()

    lane16 = lax.broadcasted_iota(jnp.int32, (16, half_y), 1)
    row16 = lax.broadcasted_iota(jnp.int32, (16, half_y), 0)

    def gram_row(i):
        def chunk(t, acc):
            at = pl.ds(pl.multiple_of(8 * t, 8), 8)
            for q in range(2):
                mine = work[i, q, at, :]
                acc = tuple(
                    acc[j] + mine * (mine if j == i else work[j, q, at, :]) for j in range(i + 1)
                )
            return acc

        acc = lax.fori_loop(
            0, rows // 8, chunk, (jnp.zeros((8, half_y), F32),) * (i + 1), unroll=4
        )
        sums = [jnp.sum(a, axis=0, keepdims=True) for a in acc]
        sums.append(jnp.zeros((16 - len(sums), half_y), F32))
        total = jnp.sum(jnp.concatenate(sums, 0), axis=1, keepdims=True)
        hit = jnp.logical_or(lane16 == i * n_vec + row16, lane16 == row16 * n_vec + i)
        hit = jnp.logical_and(hit, row16 <= i)
        return jnp.sum(jnp.where(hit, jnp.broadcast_to(total, hit.shape), 0.0), 0, keepdims=True)

    res_copy.wait()
    split_columns(n_prev)
    for c in range(comps):
        for ro in range(4):
            for p in range(2):
                for q in range(2):
                    vec[0, c, ro, p, q] = jnp.concatenate(
                        [work[n_prev, q, native(c, ro, p, h), :] for h in range(2)], 0
                    )
    zero_row = jnp.zeros((8, half_y), F32)
    send_r[0, 0, 2 * comps] = zero_row
    send_x[0, 0, 2 * comps] = zero_row
    for c in range(comps):
        for q in range(2):
            i = 2 * c + q
            send_r[0, 0, i] = jnp.where(upper, roll_s(vec[0, c, 0, 1, q], 4), vec[0, c, 0, 0, q])
            send_x[0, 0, i] = pack_x([vec[0, c, ro, 0, q] for ro in range(4)], 0)
            send_c[0, 0, i : i + 1] = vec[0, c, 0, 0, q, 0:1]

    pl.semaphore_wait(barrier, n_dev - 1)
    start_round(0)
    prev_copy.wait()
    for i in range(n_prev):
        split_columns(i)
    finish_round(0)
    for c in range(comps):
        absorb(0, c)

    total = jnp.zeros((1, half_y), F32)
    for k in range(n_steps):
        for c in range(comps):
            apply(k, c)
        start_round(k + 1)
        if k == 0:
            for i in range(n_prev + 1):
                total = total + gram_row(i)
        else:
            to_native(k)
            write_out(k)
            total = total + gram_row(n_prev + k)
        finish_round(k + 1)
        for c in range(comps):
            absorb(k + 1, c)

    to_native(n_steps)
    total = total + gram_row(n_vec - 1)
    gram_send[...] = total

    def gram_copy(d):
        return pltpu.make_async_remote_copy(
            src_ref=gram_send,
            dst_ref=gram_recv.at[d - 1],
            send_sem=gram_sems.at[0],
            recv_sem=gram_sems.at[1],
            device_id=other(d),
            device_id_type=MESH,
        )

    def scatter(d, carry):
        gram_copy(d).start()
        return carry

    lax.fori_loop(1, n_dev, scatter, 0)
    write_out(n_steps)
    for step in range(n_steps + 1):
        for d in dirs_of(step):

            @pl.when(inside(*d))
            def _(d=d, step=step):
                copy_of(step, d).wait_send()

    for i in range(2):
        pltpu.make_async_copy(gram_recv, gram_recv, gram_sems.at[i]).wait()
    full = (total + jnp.sum(gram_recv[...], axis=0)) * (1.0 / (rows * 2 * half_y * n_dev))
    for i in range(n_vec):
        line = full if i == 0 else pltpu.roll(full, half_y - i * n_vec, 1)
        gram_ref[i : i + 1, :] = line[:, :n_vec]
    for k in range(1, n_steps + 1):
        out_copy(k).wait()


def on_device(residual, prev_basis, layer_ids, viscosity, shifts):
    n_lat = lax.axis_size("lat")
    n_rad = lax.axis_size("rad")
    comps, node_r, node_x, node_y = residual.shape
    n_prev = prev_basis.shape[0]
    n_steps = shifts.shape[0]
    n_vec = n_prev + n_steps + 1
    rows = comps * node_r * node_x
    half_y = node_y // 2
    assert node_r == 8 and node_x == 8 and half_y == 128
    rounds = n_steps + 1
    tile = (8, half_y)
    vmem = pltpu.VMEM
    any_spec = pl.BlockSpec(memory_space=pl.ANY)
    vmem_spec = pl.BlockSpec(memory_space=pltpu.VMEM)
    smem_spec = pl.BlockSpec(memory_space=pltpu.SMEM)
    out, gram = pl.pallas_call(
        functools.partial(kernel, n_lat, n_rad, n_steps, n_prev, comps),
        out_shape=(
            jax.ShapeDtypeStruct((n_steps, rows, node_y), F32),
            jax.ShapeDtypeStruct((n_vec, n_vec), F32),
        ),
        in_specs=[any_spec, any_spec, vmem_spec, smem_spec, smem_spec],
        out_specs=(any_spec, vmem_spec),
        scratch_shapes=[
            vmem((n_prev + 1, rows, node_y), F32),
            vmem((n_steps, rows, node_y), F32),
            vmem((n_vec, 2, rows, half_y), F32),
            vmem((2, comps, 4, 2, 2) + tile, F32),
            vmem((2, comps, 2, 2) + tile, F32),
            vmem((2, comps, 4, 2) + tile, F32),
            vmem((2, comps, 2) + tile, F32),
            vmem((2, 9) + tile, F32),
            vmem((rounds, 2, 2 * comps + 1) + tile, F32),
            vmem((rounds, 2, 2 * comps + 1) + tile, F32),
            vmem((rounds, 4) + tile, F32),
            vmem((rounds, 2, 2 * comps + 1) + tile, F32),
            vmem((rounds, 2, 2 * comps + 1) + tile, F32),
            vmem((rounds, 4) + tile, F32),
            vmem((1, half_y), F32),
            vmem((n_lat * n_rad - 1, 1, half_y), F32),
            pltpu.SemaphoreType.DMA((2,)),
            pltpu.SemaphoreType.DMA((n_steps,)),
            pltpu.SemaphoreType.DMA((rounds, 8)),
            pltpu.SemaphoreType.DMA((rounds, 8)),
            pltpu.SemaphoreType.DMA((2,)),
        ],
        compiler_params=pltpu.CompilerParams(
            collective_id=0, has_side_effects=True, vmem_limit_bytes=48 * 1024 * 1024
        ),
    )(
        residual.reshape(rows, node_y),
        prev_basis.reshape(n_prev, rows, node_y),
        layer_ids,
        viscosity,
        shifts,
    )
    return out.reshape((n_steps,) + residual.shape), gram


def solution(mesh):
    placed = (
        P(None, "rad", "lat", None),
        P(None, None, "rad", "lat", None),
        P("rad", "lat", None),
        P(),
        P(),
    )
    return jax.shard_map(
        on_device,
        mesh=mesh,
        in_specs=placed,
        out_specs=(P(None, None, "rad", "lat", None), P()),
        check_vma=False,
    )
```

```python
import functools

import jax
import jax.numpy as jnp
from jax import lax
from jax.experimental import pallas as pl
from jax.experimental.pallas import tpu as pltpu
from jax.sharding import PartitionSpec as P

MESH = pl.DeviceIdType.MESH
F32 = jnp.float32

mass = (1.0 / 36, 1.0 / 12, 1.0 / 45)
stiff = (0.0, 1.0, 4.0 / 3)

DIRS = ((-1, -1), (-1, 0), (-1, 1), (0, -1), (0, 1), (1, -1), (1, 0), (1, 1))
SLOT = {d: i for i, d in enumerate(DIRS)}
R_DIRS = {(-1, 0): 0, (1, 0): 1}
X_DIRS = {(0, -1): 0, (0, 1): 1}
C_DIRS = {(-1, -1): 0, (-1, 1): 1, (1, -1): 2, (1, 1): 3}
FIRST = ((-1, 0), (0, -1), (-1, -1))
LAST = ((1, 0), (0, 1), (1, 1))


def weight(a, b, c):
    return (
        stiff[a] * mass[b] * mass[c] + mass[a] * stiff[b] * mass[c] + mass[a] * mass[b] * stiff[c]
    )


def forward(u0, u1, u2):
    total = u0 + u2
    twice = u1 + u1
    return total + (twice + twice), u0 - u2, total - twice


def backward(m0, m1, m2):
    both = m0 + m2
    half = m0 + m0 - m2
    return both + m1, half + half, both - m1


def kernel(
    n_lat,
    n_rad,
    n_steps,
    n_prev,
    comps,
    res_ref,
    prev_ref,
    ids_hbm,
    visc_hbm,
    shift_hbm,
    out_ref,
    gram_ref,
    stage,
    back,
    ids_ref,
    visc_ref,
    shift_ref,
    work,
    vec,
    ghost_r,
    ghost_x,
    ghost_c,
    scaled,
    send_r,
    send_x,
    send_c,
    recv_r,
    recv_x,
    recv_c,
    gram_send,
    gram_recv,
    in_sem,
    out_sem,
    send_sem,
    recv_sem,
    gram_sems,
):
    n_dev = n_lat * n_rad
    lat = lax.axis_index("lat")
    rad = lax.axis_index("rad")
    me = lat * n_rad + rad
    rows = res_ref.shape[0]
    half_y = res_ref.shape[1] // 2
    n_vec = n_prev + n_steps + 1

    res_copy = pltpu.make_async_copy(res_ref, stage.at[n_prev], in_sem.at[0])
    res_copy.start()
    prev_copy = pltpu.make_async_copy(prev_ref, stage.at[pl.ds(0, n_prev)], in_sem.at[1])
    small_copies = [
        pltpu.make_async_copy(a, b, in_sem.at[2 + i])
        for i, (a, b) in enumerate(
            ((ids_hbm, ids_ref), (visc_hbm, visc_ref), (shift_hbm, shift_ref))
        )
    ]
    for copy in small_copies:
        copy.start()
    prev_copy.start()

    recv_r[...] = jnp.zeros_like(recv_r)
    recv_x[...] = jnp.zeros_like(recv_x)
    recv_c[...] = jnp.zeros_like(recv_c)

    barrier = pltpu.get_barrier_semaphore()

    def other(d):
        t = lax.rem(me + d, n_dev)
        return {"lat": t // n_rad, "rad": lax.rem(t, n_rad)}

    def greet(d, carry):
        pl.semaphore_signal(barrier, inc=1, device_id=other(d), device_id_type=MESH)
        return carry

    lax.fori_loop(1, n_dev, greet, 0)

    sub = lax.broadcasted_iota(jnp.int32, (8, half_y), 0)
    lane = lax.broadcasted_iota(jnp.int32, (8, half_y), 1)
    upper = sub >= 4
    ex = lax.rem(sub, 4)
    first_x = ex == 0
    last_x = ex == 3
    corner0 = sub == 0
    corner3 = sub == 3
    corner4 = sub == 4
    corner7 = sub == 7
    has_up = rad < n_rad - 1
    has_right = lat < n_lat - 1
    up_f = jnp.where(has_up, 1.0, 0.0).astype(F32)
    right_f = jnp.where(has_right, 1.0, 0.0).astype(F32)
    both_f = up_f * right_f

    def roll_s(v, k):
        return pltpu.roll(v, k % 8, 0)

    def keep(mask, v):
        return jnp.where(mask, v, 0.0)

    src = lax.broadcasted_iota(jnp.int32, (2 * half_y, 2 * half_y), 0)
    dst = lax.broadcasted_iota(jnp.int32, (2 * half_y, 2 * half_y), 1)
    split_perm = jnp.where(
        src == jnp.where(dst < half_y, 2 * dst, 2 * (dst - half_y) + 1), 1.0, 0.0
    ).astype(F32)
    join_perm = jnp.where(
        dst == jnp.where(src < half_y, 2 * src, 2 * (src - half_y) + 1), 1.0, 0.0
    ).astype(F32)

    def exact_dot(a, b):
        return jnp.dot(a, b, precision=lax.Precision.HIGHEST, preferred_element_type=F32)

    def split_columns(i):
        z = exact_dot(stage[i], split_perm)
        work[i, 0] = z[:, :half_y]
        work[i, 1] = z[:, half_y:]

    def native(c, ro, p, h):
        return pl.ds(c * 64 + (4 * h + ro) * 8 + p, 4, stride=2)

    kinds = {}
    for a in range(3):
        for b in range(3):
            for c in range(3):
                key = tuple(sorted((a, b, c)))
                if key != (0, 0, 0) and key not in kinds:
                    kinds[key] = len(kinds)
    def copy_of(step, c, d):
        if d in R_DIRS:
            a, b = send_r.at[step, c, R_DIRS[d]], recv_r.at[step, c, R_DIRS[d]]
        elif d in X_DIRS:
            a, b = send_x.at[step, c, X_DIRS[d]], recv_x.at[step, c, X_DIRS[d]]
        else:
            a, b = send_c.at[step, c, C_DIRS[d]], recv_c.at[step, c, C_DIRS[d]]
        return pltpu.make_async_remote_copy(
            src_ref=a,
            dst_ref=b,
            send_sem=send_sem.at[step, c, SLOT[d]],
            recv_sem=recv_sem.at[step, c, SLOT[d]],
            device_id={"lat": lat + d[1], "rad": rad + d[0]},
            device_id_type=MESH,
        )

    def inside(dr, dx):
        ok = None
        for pos, step, count in ((rad, dr, n_rad), (lat, dx, n_lat)):
            if step:
                one = (pos > 0) if step < 0 else (pos < count - 1)
                ok = one if ok is None else jnp.logical_and(ok, one)
        return ok

    order = ((-1, -1), (1, 1), (-1, 1), (1, -1), (1, 0), (-1, 0), (0, 1), (0, -1))

    def dirs_of(step):
        wanted = FIRST if step == 0 else (LAST if step == n_steps else DIRS)
        return [d for d in order if d in wanted]

    def start_round(step, c):
        for d in dirs_of(step):

            @pl.when(inside(*d))
            def _(d=d):
                copy_of(step, c, d).start()

    def finish_round(step, c):
        for d in dirs_of(step):

            @pl.when(inside(-d[0], -d[1]))
            def _(d=d):
                copy_of(step, c, d).wait_recv()

    def pack_x(vals, at):
        out = None
        for ro in range(4):
            moved = roll_s(vals[ro], ro - at)
            out = moved if out is None else jnp.where(ex == ro, moved, out)
        return out

    def apply(k, c):
        s = shift_ref[k]
        cur = k % 2
        new = 1 - cur
        u = {}
        gx = {}
        for q in range(2):
            for ro in range(4):
                gx[ro, q] = ghost_x[cur, c, ro, q]
                for p in range(2):
                    u[ro, p, q] = vec[cur, c, ro, p, q]
            gx[4, q] = jnp.where(upper, ghost_c[cur, c, q], roll_s(gx[0, q], 4))
            for p in range(2):
                u[4, p, q] = jnp.where(upper, ghost_r[cur, c, p, q], roll_s(u[0, p, q], 4))
            for ro in range(5):
                u[ro, 2, q] = jnp.where(last_x, gx[ro, q], roll_s(u[ro, 0, q], -1))
        res = {}
        for e in range(2):
            t = {}
            for p in range(3):
                for q in range(2):
                    t[0, p, q], t[1, p, q], t[2, p, q] = forward(
                        u[2 * e, p, q], u[2 * e + 1, p, q], u[2 * e + 2, p, q]
                    )
            w = {}
            for a in range(3):
                x = {}
                for q in range(2):
                    x[0, q], x[1, q], x[2, q] = forward(t[a, 0, q], t[a, 1, q], t[a, 2, q])
                for b in range(3):
                    nxt = keep(lane != half_y - 1, pltpu.roll(x[b, 0], half_y - 1, 1))
                    m = list(forward(x[b, 0], x[b, 1], nxt))
                    for j in range(3):
                        key = tuple(sorted((a, b, j)))
                        if key in kinds:
                            m[j] = m[j] * scaled[e, kinds[key]]
                        else:
                            m[j] = None
                    if m[0] is None:
                        r0 = m[1] + m[2]
                        r1 = -(m[2] + m[2])
                        r2 = m[2] - m[1]
                    else:
                        r0, r1, r2 = backward(*m)
                    x[b, 0] = r0 + keep(lane != 0, pltpu.roll(r2, 1, 1))
                    x[b, 1] = r1
                for q in range(2):
                    w[a, 0, q], w[a, 1, q], w[a, 2, q] = backward(x[0, q], x[1, q], x[2, q])
            for p in range(3):
                for q in range(2):
                    r = backward(w[0, p, q], w[1, p, q], w[2, p, q])
                    for i in range(3):
                        key = (2 * e + i, p, q)
                        res[key] = res[key] + r[i] if key in res else r[i]
        px = {}
        for q in range(2):
            for ro in range(5):
                edge = res[ro, 2, q]
                px[ro, q] = edge
                res[ro, 0, q] = res[ro, 0, q] + keep(ex != 0, roll_s(edge, 1))
            for p in range(2):
                res[0, p, q] = res[0, p, q] + keep(upper, roll_s(res[4, p, q], 4))
            px[0, q] = px[0, q] + keep(upper, roll_s(px[4, q], 4))
        step = k + 1
        last = step == n_steps
        for q in range(2):
            face = slice(8 * q, 8 * q + 8)
            edge = slice(16 + q, 17 + q)
            row = slice(q, q + 1)
            send_r[step, c, 1, face] = jnp.where(upper, res[4, 1, q], roll_s(res[4, 0, q], 4))
            send_r[step, c, 1, edge] = px[4, q][7:8]
            send_x[step, c, 1, face] = pack_x([px[ro, q] for ro in range(4)], 3)
            send_x[step, c, 1, edge] = px[4, q][7:8]
            send_c[step, c, 3, row] = px[4, q][7:8]
            if not last:
                send_r[step, c, 0, face] = jnp.where(upper, roll_s(res[0, 1, q], 4), res[0, 0, q])
                send_r[step, c, 0, edge] = px[0, q][3:4]
                send_x[step, c, 0, face] = pack_x([res[ro, 0, q] for ro in range(4)], 0)
                send_x[step, c, 0, edge] = res[4, 0, q][4:5]
                send_c[step, c, 0, row] = res[0, 0, q][0:1]
                send_c[step, c, 1, row] = px[0, q][3:4]
                send_c[step, c, 2, row] = res[4, 0, q][4:5]
            for ro in range(4):
                for p in range(2):
                    vec[new, c, ro, p, q] = res[ro, p, q] - s * u[ro, p, q]
                if not last:
                    ghost_x[new, c, ro, q] = px[ro, q] - s * gx[ro, q]
            if not last:
                for p in range(2):
                    ghost_r[new, c, p, q] = res[4, p, q] - s * u[4, p, q]
                ghost_c[new, c, q] = px[4, q] - s * gx[4, q]

    def absorb(step, c):
        new = step % 2
        first, last = step == 0, step == n_steps
        for q in range(2):
            face = slice(8 * q, 8 * q + 8)
            line = slice(16 + q, 17 + q)
            row = slice(q, q + 1)

            def spot(ref_row, mask):
                return keep(mask, jnp.broadcast_to(ref_row, (8, half_y)))

            if not first:
                from_low = recv_r[step, c, 1, face]
                from_left = recv_x[step, c, 1, face]
                corner = spot(recv_c[step, c, 3, row], corner0)
                vec[new, c, 0, 0, q] += (
                    keep(~upper, from_low) + keep(first_x, from_left) + corner
                )
                vec[new, c, 0, 1, q] += keep(~upper, roll_s(from_low, 4))
                for ro in range(1, 4):
                    vec[new, c, ro, 0, q] += keep(first_x, roll_s(from_left, -ro))
            if not last:
                from_up = recv_r[step, c, 0, face]
                from_right = recv_x[step, c, 0, face]
                add0 = keep(upper, roll_s(from_up, 4))
                add1 = keep(upper, from_up)
                edge = keep(last_x, roll_s(from_right, 3))
                far = (
                    spot(recv_r[step, c, 0, line], corner7)
                    + spot(recv_x[step, c, 0, line], corner7)
                    + spot(recv_c[step, c, 0, row], corner7)
                )
                if not first:
                    add0 = (
                        add0
                        + spot(recv_x[step, c, 1, line], corner4)
                        + spot(recv_c[step, c, 1, row], corner4)
                    )
                    edge = (
                        edge
                        + spot(recv_r[step, c, 1, line], corner3)
                        + spot(recv_c[step, c, 2, row], corner3)
                    )
                    add0 = add0 + ghost_r[new, c, 0, q]
                    add1 = add1 + ghost_r[new, c, 1, q]
                    edge = edge + ghost_x[new, c, 0, q]
                    far = far + ghost_c[new, c, q]
                ghost_r[new, c, 0, q] = add0 * up_f
                ghost_r[new, c, 1, q] = add1 * up_f
                ghost_x[new, c, 0, q] = edge * right_f
                ghost_c[new, c, q] = far * both_f
                for ro in range(1, 4):
                    edge = keep(last_x, roll_s(from_right, 3 - ro))
                    if not first:
                        edge = edge + ghost_x[new, c, ro, q]
                    ghost_x[new, c, ro, q] = edge * right_f

    def to_native(k):
        cur = k % 2
        for c in range(comps):
            for ro in range(4):
                for p in range(2):
                    for q in range(2):
                        v = vec[cur, c, ro, p, q]
                        for h in range(2):
                            work[n_prev + k, q, native(c, ro, p, h), :] = v[4 * h : 4 * h + 4]

    def out_copy(k):
        return pltpu.make_async_copy(back.at[k - 1], out_ref.at[k - 1], out_sem.at[k - 1])

    def write_out(k):
        z = jnp.concatenate([work[n_prev + k, 0], work[n_prev + k, 1]], 1)
        back[k - 1] = exact_dot(z, join_perm)
        out_copy(k).start()

    lane16 = lax.broadcasted_iota(jnp.int32, (16, half_y), 1)
    row16 = lax.broadcasted_iota(jnp.int32, (16, half_y), 0)

    def gram_row(i):
        def chunk(t, acc):
            at = pl.ds(pl.multiple_of(8 * t, 8), 8)
            for q in range(2):
                mine = work[i, q, at, :]
                acc = tuple(
                    acc[j] + mine * (mine if j == i else work[j, q, at, :]) for j in range(i + 1)
                )
            return acc

        acc = lax.fori_loop(
            0, rows // 8, chunk, (jnp.zeros((8, half_y), F32),) * (i + 1), unroll=4
        )
        sums = [jnp.sum(a, axis=0, keepdims=True) for a in acc]
        sums.append(jnp.zeros((16 - len(sums), half_y), F32))
        total = jnp.sum(jnp.concatenate(sums, 0), axis=1, keepdims=True)
        hit = jnp.logical_or(lane16 == i * n_vec + row16, lane16 == row16 * n_vec + i)
        hit = jnp.logical_and(hit, row16 <= i)
        return jnp.sum(jnp.where(hit, jnp.broadcast_to(total, hit.shape), 0.0), 0, keepdims=True)

    res_copy.wait()
    split_columns(n_prev)
    for c in range(comps):
        for ro in range(4):
            for p in range(2):
                for q in range(2):
                    vec[0, c, ro, p, q] = jnp.concatenate(
                        [work[n_prev, q, native(c, ro, p, h), :] for h in range(2)], 0
                    )
    zero_rows = jnp.zeros((2, half_y), F32)
    for c in range(comps):
        send_r[0, c, 0, 16:18] = zero_rows
        send_x[0, c, 0, 16:18] = zero_rows
        for q in range(2):
            face = slice(8 * q, 8 * q + 8)
            send_r[0, c, 0, face] = jnp.where(
                upper, roll_s(vec[0, c, 0, 1, q], 4), vec[0, c, 0, 0, q]
            )
            send_x[0, c, 0, face] = pack_x([vec[0, c, ro, 0, q] for ro in range(4)], 0)
            send_c[0, c, 0, q : q + 1] = vec[0, c, 0, 0, q, 0:1]

    pl.semaphore_wait(barrier, n_dev - 1)
    for c in range(comps):
        start_round(0, c)
    for copy in small_copies:
        copy.wait()
    for e in range(2):
        ids = jnp.concatenate([ids_ref[e], ids_ref[2 + e]], 0)
        eta = jnp.zeros((8, half_y), F32)
        for layer in range(visc_ref.shape[0]):
            eta = eta + jnp.where(ids == layer, visc_ref[layer], 0.0)
        for key, i in kinds.items():
            scaled[e, i] = eta * weight(*key)
    prev_copy.wait()
    for i in range(n_prev):
        split_columns(i)

    total = jnp.zeros((1, half_y), F32)
    for k in range(n_steps):
        for c in range(comps):
            finish_round(k, c)
            absorb(k, c)
            apply(k, c)
            start_round(k + 1, c)
        if k == 0:
            for i in range(n_prev + 1):
                total = total + gram_row(i)
        else:
            to_native(k)
            write_out(k)
            total = total + gram_row(n_prev + k)
    for c in range(comps):
        finish_round(n_steps, c)
        absorb(n_steps, c)

    to_native(n_steps)
    total = total + gram_row(n_vec - 1)
    gram_send[...] = total

    def gram_copy(d):
        return pltpu.make_async_remote_copy(
            src_ref=gram_send,
            dst_ref=gram_recv.at[d - 1],
            send_sem=gram_sems.at[0],
            recv_sem=gram_sems.at[1],
            device_id=other(d),
            device_id_type=MESH,
        )

    def scatter(d, carry):
        gram_copy(d).start()
        return carry

    lax.fori_loop(1, n_dev, scatter, 0)
    write_out(n_steps)
    for step in range(n_steps + 1):
        for c in range(comps):
            for d in dirs_of(step):

                @pl.when(inside(*d))
                def _(c=c, d=d, step=step):
                    copy_of(step, c, d).wait_send()

    for i in range(2):
        pltpu.make_async_copy(gram_recv, gram_recv, gram_sems.at[i]).wait()
    full = (total + jnp.sum(gram_recv[...], axis=0)) * (1.0 / (rows * 2 * half_y * n_dev))
    for i in range(n_vec):
        line = full if i == 0 else pltpu.roll(full, half_y - i * n_vec, 1)
        gram_ref[i : i + 1, :] = line[:, :n_vec]
    for k in range(1, n_steps + 1):
        out_copy(k).wait()


def on_device(residual, prev_basis, layer_ids, viscosity, shifts):
    n_lat = lax.axis_size("lat")
    n_rad = lax.axis_size("rad")
    comps, node_r, node_x, node_y = residual.shape
    n_prev = prev_basis.shape[0]
    n_steps = shifts.shape[0]
    n_vec = n_prev + n_steps + 1
    rows = comps * node_r * node_x
    half_y = node_y // 2
    assert node_r == 8 and node_x == 8 and half_y == 128
    rounds = n_steps + 1
    tile = (8, half_y)
    vmem = pltpu.VMEM
    hbm_spec = pl.BlockSpec(memory_space=pltpu.HBM)
    vmem_spec = pl.BlockSpec(memory_space=pltpu.VMEM)
    out, gram = pl.pallas_call(
        functools.partial(kernel, n_lat, n_rad, n_steps, n_prev, comps),
        out_shape=(
            jax.ShapeDtypeStruct((n_steps, rows, node_y), F32),
            jax.ShapeDtypeStruct((n_vec, n_vec), F32),
        ),
        in_specs=[hbm_spec] * 5,
        out_specs=(hbm_spec, vmem_spec),
        scratch_shapes=[
            vmem((n_prev + 1, rows, node_y), F32),
            vmem((n_steps, rows, node_y), F32),
            vmem(layer_ids.shape, jnp.int32),
            pltpu.SMEM(viscosity.shape, F32),
            pltpu.SMEM(shifts.shape, F32),
            vmem((n_vec, 2, rows, half_y), F32),
            vmem((2, comps, 4, 2, 2) + tile, F32),
            vmem((2, comps, 2, 2) + tile, F32),
            vmem((2, comps, 4, 2) + tile, F32),
            vmem((2, comps, 2) + tile, F32),
            vmem((2, 9) + tile, F32),
            vmem((rounds, comps, 2, 18, half_y), F32),
            vmem((rounds, comps, 2, 18, half_y), F32),
            vmem((rounds, comps, 4, 2, half_y), F32),
            vmem((rounds, comps, 2, 18, half_y), F32),
            vmem((rounds, comps, 2, 18, half_y), F32),
            vmem((rounds, comps, 4, 2, half_y), F32),
            vmem((1, half_y), F32),
            vmem((n_lat * n_rad - 1, 1, half_y), F32),
            pltpu.SemaphoreType.DMA((5,)),
            pltpu.SemaphoreType.DMA((n_steps,)),
            pltpu.SemaphoreType.DMA((rounds, comps, 8)),
            pltpu.SemaphoreType.DMA((rounds, comps, 8)),
            pltpu.SemaphoreType.DMA((2,)),
        ],
        compiler_params=pltpu.CompilerParams(
            collective_id=0, has_side_effects=True, vmem_limit_bytes=67043328
        ),
    )(
        residual.reshape(rows, node_y),
        prev_basis.reshape(n_prev, rows, node_y),
        layer_ids,
        viscosity,
        shifts,
    )
    return out.reshape((n_steps,) + residual.shape), gram


def solution(mesh):
    placed = (
        P(None, "rad", "lat", None),
        P(None, None, "rad", "lat", None),
        P("rad", "lat", None),
        P(),
        P(),
    )
    return jax.shard_map(
        on_device,
        mesh=mesh,
        in_specs=placed,
        out_specs=(P(None, None, "rad", "lat", None), P()),
        check_vma=False,
    )
```

```python
import functools

import jax
import jax.numpy as jnp
from jax import lax
from jax.experimental import pallas as pl
from jax.experimental.pallas import tpu as pltpu
from jax.sharding import PartitionSpec as P

MESH = pl.DeviceIdType.MESH
F32 = jnp.float32

mass = (1.0 / 36, 1.0 / 12, 1.0 / 45)
stiff = (0.0, 1.0, 4.0 / 3)

DIRS = ((-1, -1), (-1, 0), (-1, 1), (0, -1), (0, 1), (1, -1), (1, 0), (1, 1))
SLOT = {d: i for i, d in enumerate(DIRS)}
R_DIRS = {(-1, 0): 0, (1, 0): 1}
X_DIRS = {(0, -1): 0, (0, 1): 1}
C_DIRS = {(-1, -1): 0, (-1, 1): 1, (1, -1): 2, (1, 1): 3}
FIRST = ((-1, 0), (0, -1), (-1, -1))
LAST = ((1, 0), (0, 1), (1, 1))


def weight(a, b, c):
    return (
        stiff[a] * mass[b] * mass[c] + mass[a] * stiff[b] * mass[c] + mass[a] * mass[b] * stiff[c]
    )


def forward(u0, u1, u2):
    total = u0 + u2
    twice = u1 + u1
    return total + (twice + twice), u0 - u2, total - twice


def backward(m0, m1, m2):
    both = m0 + m2
    half = m0 + m0 - m2
    return both + m1, half + half, both - m1


def kernel(
    n_lat,
    n_rad,
    n_steps,
    n_prev,
    comps,
    res_ref,
    prev_ref,
    ids_hbm,
    visc_hbm,
    shift_hbm,
    out_ref,
    gram_ref,
    stage,
    ids_ref,
    visc_ref,
    shift_ref,
    work,
    vec,
    ghost_r,
    ghost_x,
    ghost_c,
    scaled,
    send_r,
    send_x,
    send_c,
    recv_r,
    recv_x,
    recv_c,
    gram_send,
    gram_recv,
    in_sem,
    send_sem,
    recv_sem,
    gram_sems,
):
    n_dev = n_lat * n_rad
    lat = lax.axis_index("lat")
    rad = lax.axis_index("rad")
    me = lat * n_rad + rad
    rows = res_ref.shape[0]
    half_y = res_ref.shape[1] // 2
    n_vec = n_prev + n_steps + 1

    res_copy = pltpu.make_async_copy(res_ref, stage.at[n_prev], in_sem.at[0])
    res_copy.start()
    prev_copy = pltpu.make_async_copy(prev_ref, stage.at[pl.ds(0, n_prev)], in_sem.at[1])
    small_copies = [
        pltpu.make_async_copy(a, b, in_sem.at[2 + i])
        for i, (a, b) in enumerate(
            ((ids_hbm, ids_ref), (visc_hbm, visc_ref), (shift_hbm, shift_ref))
        )
    ]
    for copy in small_copies:
        copy.start()
    prev_copy.start()

    recv_r[...] = jnp.zeros_like(recv_r)
    recv_x[...] = jnp.zeros_like(recv_x)
    recv_c[...] = jnp.zeros_like(recv_c)

    barrier = pltpu.get_barrier_semaphore()

    rad_targets = [lax.rem(rad + d, n_rad) for d in range(n_rad)]

    def each_other(visit):
        def row(ahead, carry):
            lat_target = lax.rem(lat + ahead, n_lat)
            for d in range(n_rad):
                visit(ahead * n_rad + d - 1, {"lat": lat_target, "rad": rad_targets[d]})
            return carry

        lax.fori_loop(1, n_lat, row, 0, unroll=n_lat <= 8)
        for d in range(1, n_rad):
            visit(d - 1, {"lat": lat, "rad": rad_targets[d]})

    def greet(slot, device):
        pl.semaphore_signal(barrier, inc=1, device_id=device, device_id_type=MESH)

    each_other(greet)

    sub = lax.broadcasted_iota(jnp.int32, (8, half_y), 0)
    lane = lax.broadcasted_iota(jnp.int32, (8, half_y), 1)
    upper = sub >= 4
    ex = lax.rem(sub, 4)
    first_x = ex == 0
    last_x = ex == 3
    corner0 = sub == 0
    corner3 = sub == 3
    corner4 = sub == 4
    corner7 = sub == 7
    has_up = rad < n_rad - 1
    has_right = lat < n_lat - 1
    up_f = jnp.where(has_up, 1.0, 0.0).astype(F32)
    right_f = jnp.where(has_right, 1.0, 0.0).astype(F32)
    both_f = up_f * right_f

    def roll_s(v, k):
        return pltpu.roll(v, k % 8, 0)

    def keep(mask, v):
        return jnp.where(mask, v, 0.0)

    src = lax.broadcasted_iota(jnp.int32, (2 * half_y, 2 * half_y), 0)
    dst = lax.broadcasted_iota(jnp.int32, (2 * half_y, 2 * half_y), 1)
    split_perm = jnp.where(
        src == jnp.where(dst < half_y, 2 * dst, 2 * (dst - half_y) + 1), 1.0, 0.0
    ).astype(F32)
    join_perm = jnp.where(
        dst == jnp.where(src < half_y, 2 * src, 2 * (src - half_y) + 1), 1.0, 0.0
    ).astype(F32)

    def exact_dot(a, b):
        return jnp.dot(a, b, precision=lax.Precision.HIGHEST, preferred_element_type=F32)

    def split_columns(i):
        z = exact_dot(stage[i], split_perm)
        work[i, 0] = z[:, :half_y]
        work[i, 1] = z[:, half_y:]

    def native(c, ro, p, h):
        return pl.ds(c * 64 + (4 * h + ro) * 8 + p, 4, stride=2)

    kinds = {}
    for a in range(3):
        for b in range(3):
            for c in range(3):
                key = tuple(sorted((a, b, c)))
                if key != (0, 0, 0) and key not in kinds:
                    kinds[key] = len(kinds)
    def copy_of(step, c, d):
        if d in R_DIRS:
            a, b = send_r.at[step, c, R_DIRS[d]], recv_r.at[step, c, R_DIRS[d]]
        elif d in X_DIRS:
            a, b = send_x.at[step, c, X_DIRS[d]], recv_x.at[step, c, X_DIRS[d]]
        else:
            a, b = send_c.at[step, c, C_DIRS[d]], recv_c.at[step, c, C_DIRS[d]]
        return pltpu.make_async_remote_copy(
            src_ref=a,
            dst_ref=b,
            send_sem=send_sem.at[step, c, SLOT[d]],
            recv_sem=recv_sem.at[step, c, SLOT[d]],
            device_id={"lat": lat + d[1], "rad": rad + d[0]},
            device_id_type=MESH,
        )

    def inside(dr, dx):
        ok = None
        for pos, step, count in ((rad, dr, n_rad), (lat, dx, n_lat)):
            if step:
                one = (pos > 0) if step < 0 else (pos < count - 1)
                ok = one if ok is None else jnp.logical_and(ok, one)
        return ok

    order = ((-1, -1), (1, 1), (-1, 1), (1, -1), (1, 0), (-1, 0), (0, 1), (0, -1))

    def dirs_of(step):
        wanted = FIRST if step == 0 else (LAST if step == n_steps else DIRS)
        return [d for d in order if d in wanted]

    def start_round(step, c):
        for d in dirs_of(step):

            @pl.when(inside(*d))
            def _(d=d):
                copy_of(step, c, d).start()

    def finish_round(step, c):
        for d in dirs_of(step):

            @pl.when(inside(-d[0], -d[1]))
            def _(d=d):
                copy_of(step, c, d).wait_recv()

    def pack_x(vals, at):
        out = None
        for ro in range(4):
            moved = roll_s(vals[ro], ro - at)
            out = moved if out is None else jnp.where(ex == ro, moved, out)
        return out

    def apply(k, c):
        s = shift_ref[k]
        cur = k % 2
        new = 1 - cur
        u = {}
        gx = {}
        for q in range(2):
            for ro in range(4):
                gx[ro, q] = ghost_x[cur, c, ro, q]
                for p in range(2):
                    u[ro, p, q] = vec[cur, c, ro, p, q]
            gx[4, q] = jnp.where(upper, ghost_c[cur, c, q], roll_s(gx[0, q], 4))
            for p in range(2):
                u[4, p, q] = jnp.where(upper, ghost_r[cur, c, p, q], roll_s(u[0, p, q], 4))
            for ro in range(5):
                u[ro, 2, q] = jnp.where(last_x, gx[ro, q], roll_s(u[ro, 0, q], -1))
        res = {}
        for e in range(2):
            t = {}
            for p in range(3):
                for q in range(2):
                    t[0, p, q], t[1, p, q], t[2, p, q] = forward(
                        u[2 * e, p, q], u[2 * e + 1, p, q], u[2 * e + 2, p, q]
                    )
            w = {}
            for a in range(3):
                x = {}
                for q in range(2):
                    x[0, q], x[1, q], x[2, q] = forward(t[a, 0, q], t[a, 1, q], t[a, 2, q])
                for b in range(3):
                    nxt = keep(lane != half_y - 1, pltpu.roll(x[b, 0], half_y - 1, 1))
                    m = list(forward(x[b, 0], x[b, 1], nxt))
                    for j in range(3):
                        key = tuple(sorted((a, b, j)))
                        if key in kinds:
                            m[j] = m[j] * scaled[e, kinds[key]]
                        else:
                            m[j] = None
                    if m[0] is None:
                        r0 = m[1] + m[2]
                        r1 = -(m[2] + m[2])
                        r2 = m[2] - m[1]
                    else:
                        r0, r1, r2 = backward(*m)
                    x[b, 0] = r0 + keep(lane != 0, pltpu.roll(r2, 1, 1))
                    x[b, 1] = r1
                for q in range(2):
                    w[a, 0, q], w[a, 1, q], w[a, 2, q] = backward(x[0, q], x[1, q], x[2, q])
            for p in range(3):
                for q in range(2):
                    r = backward(w[0, p, q], w[1, p, q], w[2, p, q])
                    for i in range(3):
                        key = (2 * e + i, p, q)
                        res[key] = res[key] + r[i] if key in res else r[i]
        px = {}
        for q in range(2):
            for ro in range(5):
                edge = res[ro, 2, q]
                px[ro, q] = edge
                res[ro, 0, q] = res[ro, 0, q] + keep(ex != 0, roll_s(edge, 1))
            for p in range(2):
                res[0, p, q] = res[0, p, q] + keep(upper, roll_s(res[4, p, q], 4))
            px[0, q] = px[0, q] + keep(upper, roll_s(px[4, q], 4))
        step = k + 1
        last = step == n_steps
        for q in range(2):
            face = slice(8 * q, 8 * q + 8)
            edge = slice(16 + q, 17 + q)
            row = slice(q, q + 1)
            send_r[step, c, 1, face] = jnp.where(upper, res[4, 1, q], roll_s(res[4, 0, q], 4))
            send_r[step, c, 1, edge] = px[4, q][7:8]
            send_x[step, c, 1, face] = pack_x([px[ro, q] for ro in range(4)], 3)
            send_x[step, c, 1, edge] = px[4, q][7:8]
            send_c[step, c, 3, row] = px[4, q][7:8]
            if not last:
                send_r[step, c, 0, face] = jnp.where(upper, roll_s(res[0, 1, q], 4), res[0, 0, q])
                send_r[step, c, 0, edge] = px[0, q][3:4]
                send_x[step, c, 0, face] = pack_x([res[ro, 0, q] for ro in range(4)], 0)
                send_x[step, c, 0, edge] = res[4, 0, q][4:5]
                send_c[step, c, 0, row] = res[0, 0, q][0:1]
                send_c[step, c, 1, row] = px[0, q][3:4]
                send_c[step, c, 2, row] = res[4, 0, q][4:5]
            for ro in range(4):
                for p in range(2):
                    vec[new, c, ro, p, q] = res[ro, p, q] - s * u[ro, p, q]
                if not last:
                    ghost_x[new, c, ro, q] = px[ro, q] - s * gx[ro, q]
            if not last:
                for p in range(2):
                    ghost_r[new, c, p, q] = res[4, p, q] - s * u[4, p, q]
                ghost_c[new, c, q] = px[4, q] - s * gx[4, q]

    def absorb(step, c):
        new = step % 2
        first, last = step == 0, step == n_steps
        for q in range(2):
            face = slice(8 * q, 8 * q + 8)
            line = slice(16 + q, 17 + q)
            row = slice(q, q + 1)

            def spot(ref_row, mask):
                return keep(mask, jnp.broadcast_to(ref_row, (8, half_y)))

            if not first:
                from_low = recv_r[step, c, 1, face]
                from_left = recv_x[step, c, 1, face]
                corner = spot(recv_c[step, c, 3, row], corner0)
                vec[new, c, 0, 0, q] += (
                    keep(~upper, from_low) + keep(first_x, from_left) + corner
                )
                vec[new, c, 0, 1, q] += keep(~upper, roll_s(from_low, 4))
                for ro in range(1, 4):
                    vec[new, c, ro, 0, q] += keep(first_x, roll_s(from_left, -ro))
            if not last:
                from_up = recv_r[step, c, 0, face]
                from_right = recv_x[step, c, 0, face]
                add0 = keep(upper, roll_s(from_up, 4))
                add1 = keep(upper, from_up)
                edge = keep(last_x, roll_s(from_right, 3))
                far = (
                    spot(recv_r[step, c, 0, line], corner7)
                    + spot(recv_x[step, c, 0, line], corner7)
                    + spot(recv_c[step, c, 0, row], corner7)
                )
                if not first:
                    add0 = (
                        add0
                        + spot(recv_x[step, c, 1, line], corner4)
                        + spot(recv_c[step, c, 1, row], corner4)
                    )
                    edge = (
                        edge
                        + spot(recv_r[step, c, 1, line], corner3)
                        + spot(recv_c[step, c, 2, row], corner3)
                    )
                    add0 = add0 + ghost_r[new, c, 0, q]
                    add1 = add1 + ghost_r[new, c, 1, q]
                    edge = edge + ghost_x[new, c, 0, q]
                    far = far + ghost_c[new, c, q]
                ghost_r[new, c, 0, q] = add0 * up_f
                ghost_r[new, c, 1, q] = add1 * up_f
                ghost_x[new, c, 0, q] = edge * right_f
                ghost_c[new, c, q] = far * both_f
                for ro in range(1, 4):
                    edge = keep(last_x, roll_s(from_right, 3 - ro))
                    if not first:
                        edge = edge + ghost_x[new, c, ro, q]
                    ghost_x[new, c, ro, q] = edge * right_f

    def to_native(k):
        cur = k % 2
        for c in range(comps):
            for ro in range(4):
                for p in range(2):
                    for q in range(2):
                        v = vec[cur, c, ro, p, q]
                        for h in range(2):
                            work[n_prev + k, q, native(c, ro, p, h), :] = v[4 * h : 4 * h + 4]

    def write_out(k):
        z = jnp.concatenate([work[n_prev + k, 0], work[n_prev + k, 1]], 1)
        out_ref[k - 1] = exact_dot(z, join_perm)

    lane16 = lax.broadcasted_iota(jnp.int32, (16, half_y), 1)
    row16 = lax.broadcasted_iota(jnp.int32, (16, half_y), 0)

    def gram_row(i):
        def chunk(t, acc):
            at = pl.ds(pl.multiple_of(8 * t, 8), 8)
            for q in range(2):
                mine = work[i, q, at, :]
                acc = tuple(
                    acc[j] + mine * (mine if j == i else work[j, q, at, :]) for j in range(i + 1)
                )
            return acc

        acc = lax.fori_loop(
            0, rows // 8, chunk, (jnp.zeros((8, half_y), F32),) * (i + 1), unroll=4
        )
        sums = [jnp.sum(a, axis=0, keepdims=True) for a in acc]
        sums.append(jnp.zeros((16 - len(sums), half_y), F32))
        total = jnp.sum(jnp.concatenate(sums, 0), axis=1, keepdims=True)
        hit = jnp.logical_or(lane16 == i * n_vec + row16, lane16 == row16 * n_vec + i)
        hit = jnp.logical_and(hit, row16 <= i)
        return jnp.sum(jnp.where(hit, jnp.broadcast_to(total, hit.shape), 0.0), 0, keepdims=True)

    res_copy.wait()
    split_columns(n_prev)
    for c in range(comps):
        for ro in range(4):
            for p in range(2):
                for q in range(2):
                    vec[0, c, ro, p, q] = jnp.concatenate(
                        [work[n_prev, q, native(c, ro, p, h), :] for h in range(2)], 0
                    )
    zero_rows = jnp.zeros((2, half_y), F32)
    for c in range(comps):
        send_r[0, c, 0, 16:18] = zero_rows
        send_x[0, c, 0, 16:18] = zero_rows
        for q in range(2):
            face = slice(8 * q, 8 * q + 8)
            send_r[0, c, 0, face] = jnp.where(
                upper, roll_s(vec[0, c, 0, 1, q], 4), vec[0, c, 0, 0, q]
            )
            send_x[0, c, 0, face] = pack_x([vec[0, c, ro, 0, q] for ro in range(4)], 0)
            send_c[0, c, 0, q : q + 1] = vec[0, c, 0, 0, q, 0:1]

    pl.semaphore_wait(barrier, n_dev - 1)
    for c in range(comps):
        start_round(0, c)
    for copy in small_copies:
        copy.wait()
    for e in range(2):
        ids = jnp.concatenate([ids_ref[e], ids_ref[2 + e]], 0)
        eta = jnp.zeros((8, half_y), F32)
        for layer in range(visc_ref.shape[0]):
            eta = eta + jnp.where(ids == layer, visc_ref[layer], 0.0)
        for key, i in kinds.items():
            scaled[e, i] = eta * weight(*key)
    prev_copy.wait()
    for i in range(n_prev):
        split_columns(i)

    total = jnp.zeros((1, half_y), F32)
    for k in range(n_steps):
        for c in range(comps):
            finish_round(k, c)
            absorb(k, c)
            apply(k, c)
            start_round(k + 1, c)
        if k == 0:
            for i in range(n_prev + 1):
                total = total + gram_row(i)
        else:
            to_native(k)
            write_out(k)
            total = total + gram_row(n_prev + k)
    for c in range(comps):
        finish_round(n_steps, c)
        absorb(n_steps, c)

    to_native(n_steps)
    total = total + gram_row(n_vec - 1)
    gram_send[...] = total

    def scatter(slot, device):
        pltpu.make_async_remote_copy(
            src_ref=gram_send,
            dst_ref=gram_recv.at[slot],
            send_sem=gram_sems.at[0],
            recv_sem=gram_sems.at[1],
            device_id=device,
            device_id_type=MESH,
        ).start()

    each_other(scatter)
    write_out(n_steps)
    for step in range(n_steps + 1):
        for c in range(comps):
            for d in dirs_of(step):

                @pl.when(inside(*d))
                def _(c=c, d=d, step=step):
                    copy_of(step, c, d).wait_send()

    for i in range(2):
        pltpu.make_async_copy(gram_recv, gram_recv, gram_sems.at[i]).wait()
    full = (total + jnp.sum(gram_recv[...], axis=0)) * (1.0 / (rows * 2 * half_y * n_dev))
    for i in range(n_vec):
        line = full if i == 0 else pltpu.roll(full, half_y - i * n_vec, 1)
        gram_ref[i : i + 1, :] = line[:, :n_vec]


def on_device(residual, prev_basis, layer_ids, viscosity, shifts):
    n_lat = lax.axis_size("lat")
    n_rad = lax.axis_size("rad")
    comps, node_r, node_x, node_y = residual.shape
    n_prev = prev_basis.shape[0]
    n_steps = shifts.shape[0]
    n_vec = n_prev + n_steps + 1
    rows = comps * node_r * node_x
    half_y = node_y // 2
    assert node_r == 8 and node_x == 8 and half_y == 128
    rounds = n_steps + 1
    tile = (8, half_y)
    vmem = pltpu.VMEM
    hbm_spec = pl.BlockSpec(memory_space=pltpu.HBM)
    vmem_spec = pl.BlockSpec(memory_space=pltpu.VMEM)
    out, gram = pl.pallas_call(
        functools.partial(kernel, n_lat, n_rad, n_steps, n_prev, comps),
        out_shape=(
            pltpu.VMEM((n_steps, rows, node_y), F32),
            pltpu.VMEM((n_vec, n_vec), F32),
        ),
        in_specs=[hbm_spec] * 5,
        out_specs=(vmem_spec, vmem_spec),
        scratch_shapes=[
            vmem((n_prev + 1, rows, node_y), F32),
            vmem(layer_ids.shape, jnp.int32),
            pltpu.SMEM(viscosity.shape, F32),
            pltpu.SMEM(shifts.shape, F32),
            vmem((n_vec, 2, rows, half_y), F32),
            vmem((2, comps, 4, 2, 2) + tile, F32),
            vmem((2, comps, 2, 2) + tile, F32),
            vmem((2, comps, 4, 2) + tile, F32),
            vmem((2, comps, 2) + tile, F32),
            vmem((2, 9) + tile, F32),
            vmem((rounds, comps, 2, 18, half_y), F32),
            vmem((rounds, comps, 2, 18, half_y), F32),
            vmem((rounds, comps, 4, 2, half_y), F32),
            vmem((rounds, comps, 2, 18, half_y), F32),
            vmem((rounds, comps, 2, 18, half_y), F32),
            vmem((rounds, comps, 4, 2, half_y), F32),
            vmem((1, half_y), F32),
            vmem((n_lat * n_rad - 1, 1, half_y), F32),
            pltpu.SemaphoreType.DMA((5,)),
            pltpu.SemaphoreType.DMA((rounds, comps, 8)),
            pltpu.SemaphoreType.DMA((rounds, comps, 8)),
            pltpu.SemaphoreType.DMA((2,)),
        ],
        compiler_params=pltpu.CompilerParams(
            collective_id=0, has_side_effects=True, vmem_limit_bytes=65000000
        ),
    )(
        residual.reshape(rows, node_y),
        prev_basis.reshape(n_prev, rows, node_y),
        layer_ids,
        viscosity,
        shifts,
    )
    return out.reshape((n_steps,) + residual.shape), gram


def solution(mesh):
    placed = (
        P(None, "rad", "lat", None),
        P(None, None, "rad", "lat", None),
        P("rad", "lat", None),
        P(),
        P(),
    )
    return jax.shard_map(
        on_device,
        mesh=mesh,
        in_specs=placed,
        out_specs=(P(None, None, "rad", "lat", None), P()),
        check_vma=False,
    )
```
